64 devices in a mesh: rep: 4 (over x, y), g: 16 (over z, core).
Axes of the slice: x: 2, y: 2, z: 8, core: 2. Of those that a mesh axis runs over, the one named last changes fastest.
The devices are a block of a 4x4x8 slice.
Arguments:
- hidden: bfloat16 [2048, 2048], P(('rep', 'g')), parts along dimension 0
- cache_lat: bfloat16 [2048, 512, 512], P(('rep', 'g')), parts along dimension 0
- cache_rope: bfloat16 [2048, 512, 64], P(('rep', 'g')), parts along dimension 0
- seq_lens: int32 [2048], P(('rep', 'g')), parts along dimension 0
- gain_attn: bfloat16 [2048], replicated
- w_dq: bfloat16 [2048, 768], replicated
- gain_q: bfloat16 [768], replicated
- w_uq: bfloat16 [768, 20, 192], replicated
- w_qr: bfloat16 [768, 20, 64], replicated
- w_dkv: bfloat16 [2048, 576], replicated
- gain_kv: bfloat16 [512], replicated
- w_uk: bfloat16 [512, 20, 192], replicated
- w_uv: bfloat16 [512, 20, 256], replicated
- w_o: bfloat16 [5120, 2048], replicated
- gain_mlp: bfloat16 [2048], replicated
- w_gate: bfloat16 [2048, 10240], P(None, 'g')
- w_up: bfloat16 [2048, 10240], P(None, 'g')
- w_down: bfloat16 [10240, 2048], P('g')
Outputs:
- output 1: bfloat16 [2048, 2048], P(('rep', 'g')), parts along dimension 0
- output 2: bfloat16 [2048, 512], P(('rep', 'g')), parts along dimension 0
- output 3: bfloat16 [2048, 64], P(('rep', 'g')), parts along dimension 0
There are 4 independent parts. The reference program is written for one: setup_inputs(seed, part) draws one part's arguments, and reference() takes and returns one part's arrays. A program takes and returns all parts, laid end to end along the dimension named above; an argument that names none is the same for every part.
All inputs are finite; a program needn't handle non-finite values.
Results may differ from the reference program's by a relative error of at most 0.013522.
Values are sent between devices in bfloat16 or wider.
A program may use at most 768 MiB of HBM per device.

```python
import jax
import jax.numpy as jnp
from jax import lax

BATCH_ROWS = 512
CACHE_LEN = 512
D_MODEL = 2048
NUM_HEADS = 20
Q_LORA = 768
KV_LORA = 512
ROPE_DIM = 64
NOPE_DIM = 192
V_DIM = 256
FFN_DIM = 10240


def rms_norm(values, gain_vec):
    mean_sq = jnp.mean(jnp.square(values), axis=-1, keepdims=True)
    return values * lax.rsqrt(mean_sq + 1e-6) * gain_vec.astype(jnp.float32)


def apply_rope(values, positions):
    half_dim = values.shape[-1] // 2
    inv_freq = 10000.0 ** (-jnp.arange(half_dim).astype(jnp.float32) / half_dim)
    angles = positions.astype(jnp.float32)[..., None] * inv_freq
    cos_part = jnp.cos(angles)
    sin_part = jnp.sin(angles)
    first_half = values[..., :half_dim]
    second_half = values[..., half_dim:]
    return jnp.concatenate([first_half * cos_part - second_half * sin_part, first_half * sin_part + second_half * cos_part], axis=-1)


def draw_normal(rand_key, arr_shape, spread):
    return (jax.random.normal(rand_key, arr_shape, jnp.float32) * spread).astype(jnp.bfloat16)


def draw_gain(rand_key, length):
    return jax.random.uniform(rand_key, (length,), jnp.float32, 0.5, 1.5).astype(jnp.bfloat16)


def draw_lens(rand_key):
    len_key, pick_key = jax.random.split(rand_key)
    lens_drawn = jax.random.randint(len_key, (BATCH_ROWS,), CACHE_LEN // 4, CACHE_LEN + 1, dtype=jnp.int32)
    pick_order = jax.random.permutation(pick_key, BATCH_ROWS)
    return lens_drawn.at[pick_order[0]].set(CACHE_LEN).at[pick_order[1]].set(CACHE_LEN // 4)


def setup_inputs(seed: int = 0, part: int = 0) -> dict:
    row_keys = jax.random.split(jax.random.fold_in(jax.random.key(seed), part), 4)
    weight_keys = jax.random.split(jax.random.key(seed + 1), 14)
    return {
        "hidden": draw_normal(row_keys[0], (BATCH_ROWS, D_MODEL), 1.0),
        "cache_lat": draw_normal(row_keys[1], (BATCH_ROWS, CACHE_LEN, KV_LORA), 1.0),
        "cache_rope": draw_normal(row_keys[2], (BATCH_ROWS, CACHE_LEN, ROPE_DIM), 1.0),
        "seq_lens": draw_lens(row_keys[3]),
        "gain_attn": draw_gain(weight_keys[0], D_MODEL),
        "w_dq": draw_normal(weight_keys[1], (D_MODEL, Q_LORA), D_MODEL ** -0.5),
        "gain_q": draw_gain(weight_keys[2], Q_LORA),
        "w_uq": draw_normal(weight_keys[3], (Q_LORA, NUM_HEADS, NOPE_DIM), Q_LORA ** -0.5),
        "w_qr": draw_normal(weight_keys[4], (Q_LORA, NUM_HEADS, ROPE_DIM), Q_LORA ** -0.5),
        "w_dkv": draw_normal(weight_keys[5], (D_MODEL, KV_LORA + ROPE_DIM), D_MODEL ** -0.5),
        "gain_kv": draw_gain(weight_keys[6], KV_LORA),
        "w_uk": draw_normal(weight_keys[7], (KV_LORA, NUM_HEADS, NOPE_DIM), (3 * NOPE_DIM) ** -0.5),
        "w_uv": draw_normal(weight_keys[8], (KV_LORA, NUM_HEADS, V_DIM), KV_LORA ** -0.5 * CACHE_LEN ** 0.5 / 4),
        "w_o": draw_normal(weight_keys[9], (NUM_HEADS * V_DIM, D_MODEL), (NUM_HEADS * V_DIM) ** -0.5),
        "gain_mlp": draw_gain(weight_keys[10], D_MODEL),
        "w_gate": draw_normal(weight_keys[11], (D_MODEL, FFN_DIM), D_MODEL ** -0.5),
        "w_up": draw_normal(weight_keys[12], (D_MODEL, FFN_DIM), D_MODEL ** -0.5),
        "w_down": draw_normal(weight_keys[13], (FFN_DIM, D_MODEL), FFN_DIM ** -0.5),
    }


def reference(hidden, cache_lat, cache_rope, seq_lens, gain_attn, w_dq, gain_q, w_uq, w_qr, w_dkv, gain_kv, w_uk, w_uv, w_o, gain_mlp, w_gate, w_up, w_down):
    normed = rms_norm(hidden.astype(jnp.float32), gain_attn).astype(jnp.bfloat16)
    q_in = rms_norm(jnp.dot(normed, w_dq, preferred_element_type=jnp.float32), gain_q).astype(jnp.bfloat16)
    q_nope = jnp.einsum("bq,qhn->bhn", q_in.astype(jnp.float32), w_uq.astype(jnp.float32)).astype(jnp.bfloat16)
    q_rope = apply_rope(jnp.einsum("bq,qhr->bhr", q_in.astype(jnp.float32), w_qr.astype(jnp.float32)), seq_lens[:, None]).astype(jnp.bfloat16)
    kv_raw = jnp.dot(normed, w_dkv, preferred_element_type=jnp.float32)
    new_lat = rms_norm(kv_raw[:, :KV_LORA], gain_kv).astype(jnp.bfloat16)
    new_rope = apply_rope(kv_raw[:, KV_LORA:], seq_lens).astype(jnp.bfloat16)
    q_abs = jnp.einsum("bhn,chn->bhc", q_nope.astype(jnp.float32), w_uk.astype(jnp.float32)).astype(jnp.bfloat16)
    score_scale = (NOPE_DIM + ROPE_DIM) ** -0.5
    key_pos = jnp.arange(CACHE_LEN)

    def one_row(row_data):
        q_lat, q_rot, lat_rows, rope_rows, row_len, lat_new, rope_new = row_data
        past_score = (jnp.einsum("hc,lc->hl", q_lat.astype(jnp.float32), lat_rows.astype(jnp.float32)) + jnp.einsum("hr,lr->hl", q_rot.astype(jnp.float32), rope_rows.astype(jnp.float32))) * score_scale
        own_score = (jnp.einsum("hc,c->h", q_lat.astype(jnp.float32), lat_new.astype(jnp.float32)) + jnp.einsum("hr,r->h", q_rot.astype(jnp.float32), rope_new.astype(jnp.float32))) * score_scale
        past_score = jnp.where(key_pos[None, :] < row_len, past_score, -jnp.inf)
        row_max = jnp.maximum(jnp.max(past_score, axis=-1), own_score)
        past_exp = jnp.exp(past_score - row_max[:, None])
        own_exp = jnp.exp(own_score - row_max)
        row_total = jnp.sum(past_exp, axis=-1) + own_exp
        past_prob = (past_exp / row_total[:, None]).astype(jnp.bfloat16)
        own_prob = (own_exp / row_total).astype(jnp.bfloat16)
        mixed_lat = jnp.einsum("hl,lc->hc", past_prob.astype(jnp.float32), lat_rows.astype(jnp.float32)) + own_prob.astype(jnp.float32)[:, None] * lat_new.astype(jnp.float32)[None, :]
        return mixed_lat.astype(jnp.bfloat16)

    out_lat = lax.map(one_row, (q_abs, q_rope, cache_lat, cache_rope, seq_lens, new_lat, new_rope))
    out_heads = jnp.einsum("bhc,chv->bhv", out_lat.astype(jnp.float32), w_uv.astype(jnp.float32)).astype(jnp.bfloat16)
    attn_out = jnp.dot(out_heads.reshape(BATCH_ROWS, NUM_HEADS * V_DIM), w_o, preferred_element_type=jnp.float32)
    resid_rows = (hidden.astype(jnp.float32) + attn_out).astype(jnp.bfloat16)
    mlp_in = rms_norm(resid_rows.astype(jnp.float32), gain_mlp).astype(jnp.bfloat16)
    gate_proj = jnp.dot(mlp_in, w_gate, preferred_element_type=jnp.float32)
    up_proj = jnp.dot(mlp_in, w_up, preferred_element_type=jnp.float32)
    act_vals = (jax.nn.silu(gate_proj) * up_proj).astype(jnp.bfloat16)
    out_hidden = (resid_rows.astype(jnp.float32) + jnp.dot(act_vals, w_down, preferred_element_type=jnp.float32)).astype(jnp.bfloat16)
    return out_hidden, new_lat, new_rope
```

```python
import functools

import jax
import jax.numpy as jnp
from jax import lax
from jax.experimental import pallas as pl
from jax.experimental.pallas import tpu as pltpu
from jax.sharding import PartitionSpec as P


def rms_norm(values, gain_vec):
    mean_sq = jnp.mean(jnp.square(values), axis=-1, keepdims=True)
    return values * lax.rsqrt(mean_sq + 1e-6) * gain_vec.astype(jnp.float32)


def apply_rope(values, positions):
    half_dim = values.shape[-1] // 2
    inv_freq = 10000.0 ** (-jnp.arange(half_dim).astype(jnp.float32) / half_dim)
    angles = positions.astype(jnp.float32)[..., None] * inv_freq
    cos_part = jnp.cos(angles)
    sin_part = jnp.sin(angles)
    first_half = values[..., :half_dim]
    second_half = values[..., half_dim:]
    return jnp.concatenate([first_half * cos_part - second_half * sin_part, first_half * sin_part + second_half * cos_part], axis=-1)


def attention_rows(hidden, cache_lat, cache_rope, seq_lens, gain_attn, w_dq, gain_q, w_uq, w_qr, w_dkv, gain_kv, w_uk, w_uv, w_o):
    kv_dim = w_uk.shape[0]
    cache_len = cache_lat.shape[1]
    score_scale = (w_uq.shape[2] + w_qr.shape[2]) ** -0.5
    normed = rms_norm(hidden.astype(jnp.float32), gain_attn).astype(jnp.bfloat16)
    q_in = rms_norm(jnp.dot(normed, w_dq, preferred_element_type=jnp.float32), gain_q).astype(jnp.bfloat16)
    q_nope = jnp.einsum("bq,qhn->bhn", q_in, w_uq, preferred_element_type=jnp.float32).astype(jnp.bfloat16)
    q_rope = apply_rope(jnp.einsum("bq,qhr->bhr", q_in, w_qr, preferred_element_type=jnp.float32), seq_lens[:, None]).astype(jnp.bfloat16)
    kv_raw = jnp.dot(normed, w_dkv, preferred_element_type=jnp.float32)
    new_lat = rms_norm(kv_raw[:, :kv_dim], gain_kv).astype(jnp.bfloat16)
    new_rope = apply_rope(kv_raw[:, kv_dim:], seq_lens).astype(jnp.bfloat16)
    q_abs = jnp.einsum("bhn,chn->bhc", q_nope, w_uk, preferred_element_type=jnp.float32).astype(jnp.bfloat16)
    past_score = (jnp.einsum("bhc,blc->bhl", q_abs, cache_lat, preferred_element_type=jnp.float32) + jnp.einsum("bhr,blr->bhl", q_rope, cache_rope, preferred_element_type=jnp.float32)) * score_scale
    own_score = (jnp.einsum("bhc,bc->bh", q_abs, new_lat, preferred_element_type=jnp.float32) + jnp.einsum("bhr,br->bh", q_rope, new_rope, preferred_element_type=jnp.float32)) * score_scale
    key_pos = lax.broadcasted_iota(jnp.int32, (1, 1, cache_len), 2)
    past_score = jnp.where(key_pos < seq_lens[:, None, None], past_score, -jnp.inf)
    row_max = jnp.maximum(jnp.max(past_score, axis=-1), own_score)
    past_exp = jnp.exp(past_score - row_max[..., None])
    own_exp = jnp.exp(own_score - row_max)
    row_total = jnp.sum(past_exp, axis=-1) + own_exp
    past_prob = (past_exp / row_total[..., None]).astype(jnp.bfloat16)
    own_prob = (own_exp / row_total).astype(jnp.bfloat16)
    mixed_lat = (jnp.einsum("bhl,blc->bhc", past_prob, cache_lat, preferred_element_type=jnp.float32) + own_prob.astype(jnp.float32)[..., None] * new_lat.astype(jnp.float32)[:, None, :]).astype(jnp.bfloat16)
    out_heads = jnp.einsum("bhc,chv->bhv", mixed_lat, w_uv, preferred_element_type=jnp.float32).astype(jnp.bfloat16)
    attn_out = jnp.dot(out_heads.reshape(out_heads.shape[0], -1), w_o, preferred_element_type=jnp.float32)
    resid_rows = (hidden.astype(jnp.float32) + attn_out).astype(jnp.bfloat16)
    return resid_rows, new_lat, new_rope

MESH = pl.DeviceIdType.MESH
COL_PARTS = 2


def mlp_kernel(n, resid_ref, gain_ref, wg_ref, wu_ref, wd_ref, out_ref, wgu, wdn, ag, y_own, y_snd, y_rcv, f_snd, b_snd, f_rcv, b_rcv,
               w_sem, agf_s, agf_r, agb_s, agb_r, agd_s, agd_r, yd_s, yd_r, rsf_s, rsf_r, rsb_s, rsb_r):
    me = lax.axis_index("g")
    chips = n // 2
    far = chips // 2
    rows, dim = resid_ref.shape
    ff = wg_ref.shape[1]
    chip, core = me // 2, lax.rem(me, 2)
    nxt = {"g": lax.rem(chip + 1, chips) * 2 + core}
    prv = {"g": lax.rem(chip + chips - 1, chips) * 2 + core}
    mate = {"g": chip * 2 + (1 - core)}

    weights = [
        pltpu.make_async_copy(wg_ref, wgu.at[:, 0:ff], w_sem.at[0]),
        pltpu.make_async_copy(wu_ref, wgu.at[:, ff:2 * ff], w_sem.at[1]),
        pltpu.make_async_copy(wd_ref, wdn, w_sem.at[2]),
    ]
    for copy in weights:
        copy.start()

    barrier = pltpu.get_barrier_semaphore()
    for peer in (nxt, prv, mate):
        pl.semaphore_signal(barrier, inc=1, device_id=peer, device_id_type=MESH)

    resid = resid_ref[...].astype(jnp.float32)
    mean_sq = jnp.mean(jnp.square(resid), axis=-1, keepdims=True)
    ag[0, 0:rows, :] = (resid * lax.rsqrt(mean_sq + 1e-6) * gain_ref[...].astype(jnp.float32)).astype(jnp.bfloat16)
    pl.semaphore_wait(barrier, 3)

    half = rows // 2
    cols = dim // COL_PARTS
    parts = [(h, c) for h in range(2) for c in range(COL_PARTS)]
    fwd_parts = [j for j, (h, c) in enumerate(parts) if h == 0]
    bwd_parts = [j for j, (h, c) in enumerate(parts) if h == 1]

    def before(k):
        return 0 if k == 0 else (chips - 1 if k == far else 2 * k - 1)

    def after(k):
        return 0 if k == 0 else (chips - 1 if k == far else 2 * k)

    def piece(j):
        h, c = parts[j]
        return pl.ds(h * half, half), pl.ds(c * cols, cols)

    def remote(src, dst, send, recv, peer):
        return pltpu.make_async_remote_copy(src_ref=src, dst_ref=dst, send_sem=send, recv_sem=recv, device_id=peer, device_id_type=MESH)

    def gather_fwd(k, j):
        r, c = piece(j)
        return remote(ag.at[before(k), r, c], ag.at[before(k + 1), r, c], agf_s.at[k, j], agf_r.at[k, j], nxt)

    def gather_bwd(k, j):
        r, c = piece(j)
        return remote(ag.at[after(k), r, c], ag.at[after(k + 1), r, c], agb_s.at[k, j], agb_r.at[k, j], prv)

    def gather_mate(p, h):
        src, dst = (pl.ds(0, rows), pl.ds(rows, rows)) if h is None else (pl.ds(h * half, half), pl.ds(rows + h * half, half))
        i = 0 if h is None else h
        return remote(ag.at[p, src, :], ag.at[p, dst, :], agd_s.at[p, i], agd_r.at[p, i], mate)

    def send_mate_sums(p):
        return remote(y_snd.at[p], y_rcv.at[p], yd_s.at[p], yd_r.at[p], mate)

    def reduce_fwd(k, j):
        r, c = piece(j)
        return remote(f_snd.at[k - 1, r, c], f_rcv.at[k - 1, r, c], rsf_s.at[k - 1, j], rsf_r.at[k - 1, j], nxt)

    def reduce_bwd(k, j):
        r, c = piece(j)
        return remote(b_snd.at[k - 1, r, c], b_rcv.at[k - 1, r, c], rsb_s.at[k - 1, j], rsb_r.at[k - 1, j], prv)

    started = []

    def start(copy):
        copy.start()
        started.append(copy)

    def compute(first, count):
        x = ag[first:first + count].reshape(count * 2 * rows, dim)
        gate_up = jnp.dot(x, wgu[...], preferred_element_type=jnp.float32)
        act = (jax.nn.silu(gate_up[:, 0:ff]) * gate_up[:, ff:2 * ff]).astype(jnp.bfloat16)
        y = jnp.dot(act, wdn[...], preferred_element_type=jnp.float32)
        for i in range(count):
            y_own[first + i] = y[2 * i * rows:(2 * i + 1) * rows]
            y_snd[first + i] = y[(2 * i + 1) * rows:(2 * i + 2) * rows]
            start(send_mate_sums(first + i))

    for j in range(len(parts)):
        start(gather_fwd(0, j))
        start(gather_bwd(0, j))
    start(gather_mate(0, None))
    for copy in weights:
        copy.wait()
    for k in range(1, far + 1):
        for j in range(len(parts)):
            if k < far or j in fwd_parts:
                gather_fwd(k - 1, j).wait_recv()
                if k < far - 1 or (k == far - 1 and j in fwd_parts):
                    start(gather_fwd(k, j))
            if k < far or j in bwd_parts:
                gather_bwd(k - 1, j).wait_recv()
                if k < far - 1 or (k == far - 1 and j in bwd_parts):
                    start(gather_bwd(k, j))
        if k < far:
            start(gather_mate(before(k), None))
            start(gather_mate(after(k), None))
        else:
            start(gather_mate(chips - 1, 0))
            start(gather_mate(chips - 1, 1))
        if k == 1:
            gather_mate(0, None).wait_recv()
            compute(0, 1)
        else:
            gather_mate(before(k - 1), None).wait_recv()
            gather_mate(after(k - 1), None).wait_recv()
            compute(before(k - 1), 2)
    gather_mate(chips - 1, 0).wait_recv()
    gather_mate(chips - 1, 1).wait_recv()
    compute(chips - 1, 1)

    def pair_sum(p, j):
        r, c = piece(j)
        return y_own[p, r, c] + y_rcv[p, r, c]

    for k in range(far, 0, -1):
        fp, bp = after(k), before(k)
        send_mate_sums(fp).wait_recv()
        if bp != fp:
            send_mate_sums(bp).wait_recv()
        for j in range(len(parts)):
            r, c = piece(j)
            if k < far or j in fwd_parts:
                total = pair_sum(fp, j)
                if k < far - 1 or (k == far - 1 and j in fwd_parts):
                    reduce_fwd(k + 1, j).wait_recv()
                    total = total + f_rcv[k, r, c].astype(jnp.float32)
                f_snd[k - 1, r, c] = total.astype(jnp.bfloat16)
                start(reduce_fwd(k, j))
            if k < far or j in bwd_parts:
                total = pair_sum(bp, j)
                if k < far - 1 or (k == far - 1 and j in bwd_parts):
                    reduce_bwd(k + 1, j).wait_recv()
                    total = total + b_rcv[k, r, c].astype(jnp.float32)
                b_snd[k - 1, r, c] = total.astype(jnp.bfloat16)
                start(reduce_bwd(k, j))
    send_mate_sums(0).wait_recv()
    for j in range(len(parts)):
        r, c = piece(j)
        reduce_fwd(1, j).wait_recv()
        reduce_bwd(1, j).wait_recv()
        total = pair_sum(0, j) + f_rcv[0, r, c].astype(jnp.float32) + b_rcv[0, r, c].astype(jnp.float32)
        out_ref[r, c] = (resid_ref[r, c].astype(jnp.float32) + total).astype(jnp.bfloat16)
    for copy in started:
        copy.wait_send()


def mlp_block(n, resid_rows, gain_mlp, w_gate, w_up, w_down):
    rows, dim = resid_rows.shape
    ff = w_gate.shape[1]
    chips = n // 2
    far = chips // 2
    parts = 2 * COL_PARTS
    vmem, dma = pltpu.VMEM, pltpu.SemaphoreType.DMA
    wide, narrow = jnp.float32, jnp.bfloat16
    return pl.pallas_call(
        functools.partial(mlp_kernel, n),
        out_shape=jax.ShapeDtypeStruct((rows, dim), narrow),
        in_specs=[pl.BlockSpec(memory_space=pltpu.VMEM)] * 2 + [pl.BlockSpec(memory_space=pl.ANY)] * 3,
        out_specs=pl.BlockSpec(memory_space=pltpu.VMEM),
        scratch_shapes=[
            vmem((dim, 2 * ff), narrow),
            vmem((ff, dim), narrow),
            vmem((chips, 2 * rows, dim), narrow),
            vmem((chips, rows, dim), wide),
            vmem((chips, rows, dim), wide),
            vmem((chips, rows, dim), wide),
            vmem((far, rows, dim), narrow),
            vmem((far, rows, dim), narrow),
            vmem((far, rows, dim), narrow),
            vmem((far, rows, dim), narrow),
            dma((3,)),
            dma((far, parts)), dma((far, parts)), dma((far, parts)), dma((far, parts)),
            dma((chips, 2)), dma((chips, 2)), dma((chips,)), dma((chips,)),
            dma((far, parts)), dma((far, parts)), dma((far, parts)), dma((far, parts)),
        ],
        compiler_params=pltpu.CompilerParams(collective_id=0, has_side_effects=True),
        cost_estimate=pl.CostEstimate(flops=6 * n * rows * dim * ff, bytes_accessed=6 * dim * ff, transcendentals=0),
        name="mlp_ring",
    )(resid_rows, gain_mlp.reshape(1, dim), w_gate, w_up, w_down)


def solution(mesh):
    row_spec = P(("rep", "g"))
    full_spec = P()
    in_specs = (row_spec, row_spec, row_spec, row_spec, full_spec, full_spec, full_spec, full_spec, full_spec, full_spec, full_spec, full_spec, full_spec, full_spec, full_spec, P(None, "g"), P(None, "g"), P("g", None))

    def local_step(hidden, cache_lat, cache_rope, seq_lens, gain_attn, w_dq, gain_q, w_uq, w_qr, w_dkv, gain_kv, w_uk, w_uv, w_o, gain_mlp, w_gate, w_up, w_down):
        resid_rows, new_lat, new_rope = attention_rows(hidden, cache_lat, cache_rope, seq_lens, gain_attn, w_dq, gain_q, w_uq, w_qr, w_dkv, gain_kv, w_uk, w_uv, w_o)
        out_hidden = mlp_block(mesh.shape["g"], resid_rows, gain_mlp, w_gate, w_up, w_down)
        return out_hidden, new_lat, new_rope

    return jax.shard_map(local_step, mesh=mesh, in_specs=in_specs, out_specs=(row_spec, row_spec, row_spec), check_vma=False)
```
